16 devices in a mesh: dp: 2 (over y, z), tp: 8 (over x, core).
Axes of the slice: x: 4, y: 2, z: 1, core: 2. Of those that a mesh axis runs over, the one named last changes fastest.
The devices are a block of a 4x4x8 slice.
Arguments:
- x: bfloat16 [4096, 5120], P('dp'), parts along dimension 0
- w_gate: bfloat16 [5120, 32768], P(None, 'tp')
- w_up: bfloat16 [5120, 32768], P(None, 'tp')
- w_down: bfloat16 [32768, 5120], P('tp')
Outputs:
- output: bfloat16 [4096, 5120], P('dp'), parts along dimension 0
There are 2 independent parts. The reference program is written for one: setup_inputs(seed, part) draws one part's arguments, and reference() takes and returns one part's arrays. A program takes and returns all parts, laid end to end along the dimension named above; an argument that names none is the same for every part.
All inputs are finite; a program needn't handle non-finite values.
Results may differ from the reference program's by a relative error of at most 0.016.
Values are sent between devices in bfloat16 or wider.
A program may use at most 768 MiB of HBM per device.

```python
import jax
import jax.numpy as jnp

ROWS = 2048
D = 5120
FF = 32768


def setup_inputs(seed: int = 0, part: int = 0) -> dict:
    kx, kg, ku, kd = jax.random.split(jax.random.key(seed), 4)
    drawn = {
        "x": jax.random.normal(jax.random.fold_in(kx, part), (ROWS, D), jnp.float32),
        "w_gate": jax.random.normal(kg, (D, FF), jnp.float32) * D**-0.5,
        "w_up": jax.random.normal(ku, (D, FF), jnp.float32) * D**-0.5,
        "w_down": jax.random.normal(kd, (FF, D), jnp.float32) * FF**-0.5,
    }
    return {k: v.astype(jnp.bfloat16) for k, v in drawn.items()}


def reference(x, w_gate, w_up, w_down):
    gate = jnp.dot(x, w_gate, preferred_element_type=jnp.float32)
    up = jnp.dot(x, w_up, preferred_element_type=jnp.float32)
    hidden = (jax.nn.silu(gate) * up).astype(jnp.bfloat16)
    return jnp.dot(hidden, w_down, preferred_element_type=jnp.float32).astype(jnp.bfloat16)
```

```python
import functools

import jax
import jax.numpy as jnp
from jax import lax
from jax.experimental import pallas as pl
from jax.experimental.pallas import tpu as pltpu
from jax.sharding import PartitionSpec as P

CHUNK = 512
TILE = 512
MESH = pl.DeviceIdType.MESH
F32, BF16 = jnp.float32, jnp.bfloat16


def kernel(
    n, x_hbm, wg_hbm, wu_hbm, wd_hbm, y_hbm, far_hbm,
    x_buf, w_buf, hid, term, first, got, done,
    x_sem, w_sem, far_send, far_recv, hid_send, hid_recv,
    rs_send, rs_recv, ag_send, ag_recv, twin_send, local_sem, late_send, late_recv,
):
    ring = n // 2
    rows, depth = x_hbm.shape
    width = wg_hbm.shape[1]
    half = depth // 2
    chunks, ups, downs = rows // CHUNK, width // TILE, half // TILE
    steps = ups + downs
    piece, lanes = CHUNK // ring, TILE // 2

    me = lax.axis_index("tp")
    chip, core = me // 2, me % 2
    twin = me + 1 - 2 * core
    right, left = (me + 2) % n, (me + n - 2) % n
    towards = (right, left)

    barrier = pltpu.get_barrier_semaphore()
    for peer in (left, right, twin):
        pl.semaphore_signal(barrier, inc=1, device_id={"tp": peer}, device_id_type=MESH)
    pl.semaphore_wait(barrier, 3)

    def remote(src, dst, send, recv, peer):
        return pltpu.make_async_remote_copy(
            src_ref=src, dst_ref=dst, send_sem=send, recv_sem=recv,
            device_id={"tp": peer}, device_id_type=MESH,
        )

    def far_copy(u):
        cols = pl.multiple_of((1 - core) * half + u * TILE, TILE)
        return remote(
            wd_hbm.at[:, pl.ds(cols, TILE)], far_hbm.at[:, pl.ds(pl.multiple_of(u * TILE, TILE), TILE)],
            far_send.at[u], far_recv.at[u], twin,
        )

    def x_copy(k):
        at = pl.multiple_of(k * CHUNK, CHUNK)
        return pltpu.make_async_copy(x_hbm.at[pl.ds(at, CHUNK), :], x_buf, x_sem)

    def up_copies(i, slot):
        cols = pl.ds(pl.multiple_of(i * TILE, TILE), TILE)
        return (
            pltpu.make_async_copy(wg_hbm.at[:, cols], w_buf.at[slot, pl.ds(0, depth)], w_sem.at[slot, 0]),
            pltpu.make_async_copy(wu_hbm.at[:, cols], w_buf.at[slot, pl.ds(depth, depth)], w_sem.at[slot, 1]),
        )

    def down_copies(u, slot):
        cols = pl.ds(pl.multiple_of(core * half + u * TILE, TILE), TILE)
        far = pl.ds(pl.multiple_of(u * TILE, TILE), TILE)
        return (
            pltpu.make_async_copy(wd_hbm.at[:, cols], w_buf.at[slot, pl.ds(0, width)], w_sem.at[slot, 0]),
            pltpu.make_async_copy(far_hbm.at[:, far], w_buf.at[slot, pl.ds(width, width)], w_sem.at[slot, 1]),
        )

    def start(copies):
        for copy in copies:
            copy.start()

    def wait(copies):
        for copy in copies:
            copy.wait()

    def start_down(k, u, slot):
        @pl.when(k == 0)
        def _():
            far_copy(u).wait()

        start(down_copies(u, slot))

    def spot(k, u, d, owner):
        at = pl.multiple_of(k * CHUNK + owner * piece, piece)
        cols = pl.multiple_of(core * half + u * TILE + d * lanes, lanes)
        return y_hbm.at[pl.ds(at, piece), pl.ds(cols, lanes)]

    def owner_of(d, s):
        return (chip + ring - 1 - s) % ring if d == 0 else (chip + 1 + s) % ring

    def rs_copy(d, u, s):
        src = first.at[d, u] if s == 0 else got.at[d, u, s - 1]
        return remote(src, got.at[d, u, s], rs_send.at[d, u, s], rs_recv.at[d, u, s], towards[d])

    def ag_copy(k, d, u, s):
        owner = owner_of(d, ring - 1 + s)
        src = done.at[d, u] if s == 0 else spot(k, u, d, owner)
        return remote(src, spot(k, u, d, owner), ag_send.at[d, u, s], ag_recv.at[d, u, s], towards[d])

    def twin_copy(k, d, u, s):
        owner = owner_of(d, ring - 1 + s)
        src = done.at[d, u] if s == 0 else spot(k, u, d, owner)
        send = twin_send.at[d, u] if s == 0 else late_send
        return remote(src, spot(k, u, d, owner), send, late_recv, twin)

    def local_copy(k, d, u):
        return pltpu.make_async_copy(done.at[d, u], spot(k, u, d, chip), local_sem.at[d, u])

    def own_term(d, u, s):
        at = pl.multiple_of(owner_of(d, s) * piece, piece)
        return term[u, pl.ds(at, piece), pl.ds(d * lanes, lanes)]

    last = ring - 1

    def event(k, u, s):
        if s == 0:
            for d in range(2):
                first[d, u] = own_term(d, u, 0).astype(BF16)
            for d in range(2):
                rs_copy(d, u, 0).start()
        elif s < last:
            for d in range(2):
                rs_copy(d, u, s - 1).wait_recv()
                got[d, u, s - 1] = (got[d, u, s - 1].astype(F32) + own_term(d, u, s)).astype(BF16)
            for d in range(2):
                rs_copy(d, u, s).start()
        elif s == last:
            for d in range(2):
                rs_copy(d, u, s - 1).wait_recv()
                done[d, u] = (got[d, u, s - 1].astype(F32) + own_term(d, u, s)).astype(BF16)
                for r in range(last):
                    rs_copy(d, u, r).wait_send()
            for d in range(2):
                ag_copy(k, d, u, 0).start()
                twin_copy(k, d, u, 0).start()
                local_copy(k, d, u).start()
        else:
            for d in range(2):
                ag_copy(k, d, u, s - last - 1).wait_recv()
                if s < 2 * last:
                    ag_copy(k, d, u, s - last).start()
                twin_copy(k, d, u, s - last).start()
            if s == 2 * last:
                for d in range(2):
                    for r in range(last):
                        ag_copy(k, d, u, r).wait_send()
                    twin_copy(k, d, u, 0).wait_send()
                    local_copy(k, d, u).wait()

    def events(k, tau):
        for s in range(2 * last, -1, -1):
            u = tau - 2 * s

            @pl.when((u >= 0) & (u < downs))
            def _(u=u, s=s):
                event(k, u, s)

    start(up_copies(0, 0))
    x_copy(0).start()
    for u in range(downs):
        far_copy(u).start()

    def chunk_body(k, _):
        x_copy(k).wait()
        par = k % 2
        hid_here = hid.at[par]

        def hid_copy(i):
            own = pl.ds(pl.multiple_of(i * TILE, TILE), TILE)
            far = pl.ds(pl.multiple_of(width + i * TILE, TILE), TILE)
            return remote(hid.at[par, :, own], hid.at[par, :, far], hid_send.at[par], hid_recv.at[par], twin)

        def up_body(i, _):
            slot = (k * steps + i) % 2
            wait(up_copies(i, slot))

            @pl.when(i < ups - 1)
            def _():
                start(up_copies(i + 1, 1 - slot))

            @pl.when(i == ups - 1)
            def _():
                start_down(k, 0, 1 - slot)

            gate = jnp.dot(x_buf[...], w_buf[slot, pl.ds(0, depth)], preferred_element_type=F32)
            up = jnp.dot(x_buf[...], w_buf[slot, pl.ds(depth, depth)], preferred_element_type=F32)
            hid[par, :, pl.ds(pl.multiple_of(i * TILE, TILE), TILE)] = (jax.nn.silu(gate) * up).astype(BF16)

            @pl.when(k > 0)
            def _():
                events(k - 1, i + downs)

            hid_copy(i).start()
            return _

        lax.fori_loop(0, ups, up_body, None)

        @pl.when(k < chunks - 1)
        def _():
            x_copy(k + 1).start()

        whole = remote(
            hid.at[par, :, pl.ds(0, width)], hid.at[par, :, pl.ds(width, width)],
            hid_send.at[par], hid_recv.at[par], twin,
        )
        whole.wait()

        def down_body(u, _):
            slot = (k * steps + ups + u) % 2
            wait(down_copies(u, slot))

            @pl.when(u < downs - 1)
            def _():
                start_down(k, u + 1, 1 - slot)

            @pl.when((u == downs - 1) & (k < chunks - 1))
            def _():
                start(up_copies(0, 1 - slot))

            term[u] = jnp.dot(hid_here[...], w_buf[slot, pl.ds(0, 2 * width)], preferred_element_type=F32)

            @pl.when(k > 0)
            def _():
                events(k - 1, u + steps)

            events(k, u)
            return _

        lax.fori_loop(0, downs, down_body, None)
        return _

    lax.fori_loop(0, chunks, chunk_body, None)

    def tail(tau, _):
        events(chunks - 1, tau)
        return _

    lax.fori_loop(downs, downs + 4 * last, tail, None)

    share = (rows // ring) * last
    pltpu.make_async_copy(
        y_hbm.at[pl.ds(0, share), pl.ds(0, half)], y_hbm.at[pl.ds(0, share), pl.ds(0, half)], late_send
    ).wait()
    pltpu.make_async_copy(y_hbm.at[:, pl.ds(0, half)], y_hbm.at[:, pl.ds(0, half)], late_recv).wait()


def solution(mesh):
    n = mesh.shape["tp"]
    ring = n // 2

    def step(x, w_gate, w_up, w_down):
        rows, depth = x.shape
        width = w_gate.shape[1]
        half = depth // 2
        downs = half // TILE
        piece, lanes = CHUNK // ring, TILE // 2
        dma = pltpu.SemaphoreType.DMA
        y, _ = pl.pallas_call(
            functools.partial(kernel, n),
            name="mlp",
            out_shape=(
                jax.ShapeDtypeStruct((rows, depth), BF16),
                jax.ShapeDtypeStruct((width, half), BF16),
            ),
            in_specs=[pl.BlockSpec(memory_space=pl.ANY)] * 4,
            out_specs=[pl.BlockSpec(memory_space=pl.ANY)] * 2,
            scratch_shapes=[
                pltpu.VMEM((CHUNK, depth), BF16),
                pltpu.VMEM((2, 2 * depth, TILE), BF16),
                pltpu.VMEM((2, CHUNK, 2 * width), BF16),
                pltpu.VMEM((downs, CHUNK, TILE), F32),
                pltpu.VMEM((2, downs, piece, lanes), BF16),
                pltpu.VMEM((2, downs, ring - 1, piece, lanes), BF16),
                pltpu.VMEM((2, downs, piece, lanes), BF16),
                dma,
                dma((2, 2)),
                dma((downs,)),
                dma((downs,)),
                dma((2,)),
                dma((2,)),
                dma((2, downs, ring - 1)),
                dma((2, downs, ring - 1)),
                dma((2, downs, ring - 1)),
                dma((2, downs, ring - 1)),
                dma((2, downs)),
                dma((2, downs)),
                dma,
                dma,
            ],
            compiler_params=pltpu.CompilerParams(
                collective_id=0, has_side_effects=True, vmem_limit_bytes=67_043_328
            ),
            cost_estimate=pl.CostEstimate(
                flops=6 * rows * depth * width,
                bytes_accessed=2 * (2 * rows * depth + 12 * depth * width),
                transcendentals=rows * width,
            ),
        )(x, w_gate, w_up, w_down)
        return y

    return jax.shard_map(
        step,
        mesh=mesh,
        in_specs=(P("dp", None), P(None, "tp"), P(None, "tp"), P("tp", None)),
        out_specs=P("dp", None),
        check_vma=False,
    )
```

```python
import functools

import jax
import jax.numpy as jnp
from jax import lax
from jax.experimental import pallas as pl
from jax.experimental.pallas import tpu as pltpu
from jax.sharding import PartitionSpec as P

TILE = 512
MESH = pl.DeviceIdType.MESH
F32, BF16 = jnp.float32, jnp.bfloat16


def split(rows):
    big = rows * 9 // 32
    return big, rows // big, rows % big


def kernel(
    n, x_hbm, wg_hbm, wu_hbm, wd_hbm, y_hbm, far_hbm,
    x_buf, w_buf, hid, term, first, got1, second, got2, done,
    x_sem, w_sem, far_send, far_recv, hid_send, hid_recv,
    send1, recv1, send2, recv2, back2_send, back2_recv, back1_send, back1_recv,
    twin_send, local_sem, late_send, late_recv,
):
    rows, depth = x_hbm.shape
    width = wg_hbm.shape[1]
    half = depth // 2
    big, chunks, small = split(rows)
    ups, downs = width // TILE, half // TILE
    steps = ups + downs
    lanes = TILE // 2

    me = lax.axis_index("tp")
    chip, core = me // 2, me % 2
    twin = me + 1 - 2 * core
    inner, outer = ((chip + 1) // 2) % 2, chip // 2
    near, wrap = 2 * (chip + 1 - 2 * (chip % 2)) + core, 2 * (n // 2 - 1 - chip) + core
    keep, pick = (inner, outer), (outer, inner)
    peer1, peer2 = (near, wrap), (wrap, near)

    barrier = pltpu.get_barrier_semaphore()
    for peer in (near, wrap, twin):
        pl.semaphore_signal(barrier, inc=1, device_id={"tp": peer}, device_id_type=MESH)
    pl.semaphore_wait(barrier, 3)

    def remote(src, dst, send, recv, peer):
        return pltpu.make_async_remote_copy(
            src_ref=src, dst_ref=dst, send_sem=send, recv_sem=recv,
            device_id={"tp": peer}, device_id_type=MESH,
        )

    def tile(i):
        return pl.ds(pl.multiple_of(i * TILE, TILE), TILE)

    def far_copy(u):
        cols = pl.ds(pl.multiple_of((1 - core) * half + u * TILE, TILE), TILE)
        return remote(wd_hbm.at[:, cols], far_hbm.at[:, tile(u)], far_send.at[u], far_recv.at[u], twin)

    def x_copy(row, size):
        at = pl.multiple_of(row, 64)
        return pltpu.make_async_copy(x_hbm.at[pl.ds(at, size), :], x_buf.at[pl.ds(0, size)], x_sem)

    def up_copies(i, slot):
        return (
            pltpu.make_async_copy(wg_hbm.at[:, tile(i)], w_buf.at[slot, pl.ds(0, depth)], w_sem.at[slot, 0]),
            pltpu.make_async_copy(wu_hbm.at[:, tile(i)], w_buf.at[slot, pl.ds(depth, depth)], w_sem.at[slot, 1]),
        )

    def down_copies(u, slot):
        cols = pl.ds(pl.multiple_of(core * half + u * TILE, TILE), TILE)
        return (
            pltpu.make_async_copy(wd_hbm.at[:, cols], w_buf.at[slot, pl.ds(0, width)], w_sem.at[slot, 0]),
            pltpu.make_async_copy(far_hbm.at[:, tile(u)], w_buf.at[slot, pl.ds(width, width)], w_sem.at[slot, 1]),
        )

    def start(copies):
        for copy in copies:
            copy.start()

    def wait(copies):
        for copy in copies:
            copy.wait()

    def event(row, size, u, s):
        piece = size // 4

        def rows_of(h, q):
            return pl.multiple_of((2 * h + q) * piece, 16)

        def spot(d, h, q, count=1):
            cols = pl.multiple_of(core * half + u * TILE + d * lanes, lanes)
            return y_hbm.at[pl.ds(pl.multiple_of(row + (2 * h + q) * piece, 16), count * piece), pl.ds(cols, lanes)]

        def own(d, h, q, count=1):
            return term[u, pl.ds(rows_of(h, q), count * piece), pl.ds(d * lanes, lanes)]

        def part(d, q):
            return got1[d, u, pl.ds(pl.multiple_of(q * piece, 16), piece)].astype(F32)

        def out1(d):
            cut = pl.ds(0, 2 * piece)
            return remote(first.at[d, u, cut], got1.at[d, u, cut], send1.at[d, u], recv1.at[d, u], peer1[d])

        def out2(d):
            cut = pl.ds(0, piece)
            return remote(second.at[d, u, cut], got2.at[d, u, cut], send2.at[d, u], recv2.at[d, u], peer2[d])

        def mine(d):
            return done.at[d, u, pl.ds(0, piece)], spot(d, keep[d], pick[d])

        def back2(d):
            return remote(*mine(d), back2_send.at[d, u], back2_recv.at[d, u], peer2[d])

        def back1(d, q):
            src, dst = mine(d)
            if q:
                src = dst = spot(d, keep[d], 1 - pick[d])
            return remote(src, dst, back1_send.at[d, u, q], back1_recv.at[d, u, q], peer1[d])

        def to_twin(d):
            return remote(*mine(d), twin_send.at[d, u], late_recv, twin)

        def local(d):
            return pltpu.make_async_copy(*mine(d), local_sem.at[d, u])

        if s == 0:
            for d in range(2):
                first[d, u, pl.ds(0, 2 * piece)] = own(d, 1 - keep[d], 0, 2).astype(BF16)
            for d in range(2):
                out1(d).start()
        elif s == 1:
            for d in range(2):
                out1(d).wait_recv()
                q = 1 - pick[d]
                second[d, u, pl.ds(0, piece)] = (part(d, q) + own(d, keep[d], q)).astype(BF16)
            for d in range(2):
                out2(d).start()
        elif s == 2:
            for d in range(2):
                out2(d).wait_recv()
                total = part(d, pick[d]) + own(d, keep[d], pick[d]) + got2[d, u, pl.ds(0, piece)].astype(F32)
                done[d, u, pl.ds(0, piece)] = total.astype(BF16)
            for d in range(2):
                back2(d).start()
                back1(d, 0).start()
                to_twin(d).start()
                local(d).start()
        elif s == 3:
            for d in range(2):
                back2(d).wait_recv()
                back1(d, 1).start()
                here = spot(d, keep[d], 1 - pick[d])
                remote(here, here, late_send, late_recv, twin).start()
        else:
            for d in range(2):
                back1(d, 0).wait_recv()
                back1(d, 1).wait_recv()
                here = spot(d, 1 - keep[d], 0, 2)
                remote(here, here, late_send, late_recv, twin).start()
            for d in range(2):
                out1(d).wait_send()
                out2(d).wait_send()
                back2(d).wait_send()
                back1(d, 0).wait_send()
                back1(d, 1).wait_send()
                to_twin(d).wait_send()
                local(d).wait()

    def events(row, size, tau):
        for s in range(4, -1, -1):
            u = tau - 2 * s

            @pl.when((u >= 0) & (u < downs))
            def _(u=u, s=s):
                event(row, size, u, s)

    def chunk(k, row, size, before, after):
        x_copy(row, size).wait()
        par = k % 2
        base = k * steps
        here = pl.ds(0, size)

        def hid_copy(i):
            far = pl.ds(pl.multiple_of(width + i * TILE, TILE), TILE)
            return remote(
                hid.at[par, here, tile(i)], hid.at[par, here, far], hid_send.at[par], hid_recv.at[par], twin
            )

        def next_down(u, slot):
            @pl.when(k == 0)
            def _():
                far_copy(u).wait()

            start(down_copies(u, slot))

        def up_body(i, _):
            slot = (base + i) % 2
            wait(up_copies(i, slot))

            @pl.when(i < ups - 1)
            def _():
                start(up_copies(i + 1, 1 - slot))

            @pl.when(i == ups - 1)
            def _():
                next_down(0, 1 - slot)

            gate = jnp.dot(x_buf[here], w_buf[slot, pl.ds(0, depth)], preferred_element_type=F32)
            up = jnp.dot(x_buf[here], w_buf[slot, pl.ds(depth, depth)], preferred_element_type=F32)
            hid[par, here, tile(i)] = (jax.nn.silu(gate) * up).astype(BF16)
            before(i + downs)
            hid_copy(i).start()
            return _

        lax.fori_loop(0, ups, up_body, None)

        def down_step(u, lead):
            slot = (base + ups + u) % 2
            wait(down_copies(u, slot))
            if lead:
                next_down(u + 1, 1 - slot)
                if after is not None:
                    after()
                term[u, here] = jnp.dot(
                    hid[par, here, pl.ds(0, width)], w_buf[slot, pl.ds(0, width)], preferred_element_type=F32
                )
                remote(
                    hid.at[par, here, pl.ds(0, width)], hid.at[par, here, pl.ds(width, width)],
                    hid_send.at[par], hid_recv.at[par], twin,
                ).wait()
                term[u, here] += jnp.dot(
                    hid[par, here, pl.ds(width, width)], w_buf[slot, pl.ds(width, width)],
                    preferred_element_type=F32,
                )
            else:
                @pl.when(u < downs - 1)
                def _():
                    next_down(u + 1, 1 - slot)

                if after is not None:
                    @pl.when(u == downs - 1)
                    def _():
                        start(up_copies(0, 1 - slot))

                term[u, here] = jnp.dot(
                    hid[par, here], w_buf[slot, pl.ds(0, 2 * width)], preferred_element_type=F32
                )
            events(row, size, u)

        down_step(0, True)

        def down_body(u, _):
            down_step(u, False)
            return _

        lax.fori_loop(1, downs, down_body, None)

    start(up_copies(0, 0))
    x_copy(0, big).start()
    for u in range(downs):
        far_copy(u).start()

    def chunk_body(k, _):
        row = k * big

        def before(tau):
            @pl.when(k > 0)
            def _():
                events(row - big, big, tau)

        def after():
            @pl.when(k < chunks - 1)
            def _():
                x_copy(row + big, big).start()

            @pl.when(k == chunks - 1)
            def _():
                x_copy(row + big, small).start()

        chunk(k, row, big, before, after)
        return _

    lax.fori_loop(0, chunks, chunk_body, None)
    row = chunks * big
    chunk(chunks, row, small, lambda tau: events(row - big, big, tau), None)

    def tail(tau, _):
        events(row, small, tau)
        return _

    lax.fori_loop(downs, downs + 8, tail, None)

    share = rows // 4 * 3
    sent = y_hbm.at[pl.ds(0, share), pl.ds(0, half)]
    pltpu.make_async_copy(sent, sent, late_send).wait()
    whole = y_hbm.at[:, pl.ds(0, half)]
    pltpu.make_async_copy(whole, whole, late_recv).wait()


def solution(mesh):
    n = mesh.shape["tp"]

    def step(x, w_gate, w_up, w_down):
        rows, depth = x.shape
        width = w_gate.shape[1]
        half = depth // 2
        downs = half // TILE
        big = split(rows)[0]
        piece, lanes = big // 4, TILE // 2
        dma = pltpu.SemaphoreType.DMA
        y, _ = pl.pallas_call(
            functools.partial(kernel, n),
            name="mlp",
            out_shape=(
                jax.ShapeDtypeStruct((rows, depth), BF16),
                jax.ShapeDtypeStruct((width, half), BF16),
            ),
            in_specs=[pl.BlockSpec(memory_space=pl.ANY)] * 4,
            out_specs=[pl.BlockSpec(memory_space=pl.ANY)] * 2,
            scratch_shapes=[
                pltpu.VMEM((big, depth), BF16),
                pltpu.VMEM((2, 2 * depth, TILE), BF16),
                pltpu.VMEM((2, big, 2 * width), BF16),
                pltpu.VMEM((downs, big, TILE), F32),
                pltpu.VMEM((2, downs, 2 * piece, lanes), BF16),
                pltpu.VMEM((2, downs, 2 * piece, lanes), BF16),
                pltpu.VMEM((2, downs, piece, lanes), BF16),
                pltpu.VMEM((2, downs, piece, lanes), BF16),
                pltpu.VMEM((2, downs, piece, lanes), BF16),
                dma,
                dma((2, 2)),
                dma((downs,)),
                dma((downs,)),
                dma((2,)),
                dma((2,)),
                dma((2, downs)),
                dma((2, downs)),
                dma((2, downs)),
                dma((2, downs)),
                dma((2, downs)),
                dma((2, downs)),
                dma((2, downs, 2)),
                dma((2, downs, 2)),
                dma((2, downs)),
                dma((2, downs)),
                dma,
                dma,
            ],
            compiler_params=pltpu.CompilerParams(
                collective_id=0, has_side_effects=True, vmem_limit_bytes=67_043_328
            ),
            cost_estimate=pl.CostEstimate(
                flops=6 * rows * depth * width,
                bytes_accessed=2 * (2 * rows * depth + 12 * depth * width),
                transcendentals=rows * width,
            ),
        )(x, w_gate, w_up, w_down)
        return y

    return jax.shard_map(
        step,
        mesh=mesh,
        in_specs=(P("dp", None), P(None, "tp"), P(None, "tp"), P("tp", None)),
        out_specs=P("dp", None),
        check_vma=False,
    )
```

```python
import functools

import jax
import jax.numpy as jnp
from jax import lax
from jax.experimental import pallas as pl
from jax.experimental.pallas import tpu as pltpu
from jax.sharding import PartitionSpec as P

TILE = 512
MESH = pl.DeviceIdType.MESH
F32, BF16 = jnp.float32, jnp.bfloat16


SHARES = ((9, 2), (8, 1), (6, 1))
BLOCKS = 16
GAP, LAST_GAP = 3, 2


def split(rows):
    return [(rows * share // 32, count) for share, count in SHARES]


def kernel(
    n, x_hbm, wg_hbm, wu_hbm, wd_hbm, y_hbm, far_hbm,
    x_buf, w_buf, hid, far_hid, term, first, got1, second, got2, done,
    x_sem, w_sem, far_send, far_recv, hid_send, hid_recv,
    send1, recv1, send2, recv2, back2_send, back2_recv, back1_send, back1_recv,
    local_sem, late_send, late_recv,
):
    rows, depth = x_hbm.shape
    width = wg_hbm.shape[1]
    half = depth // 2
    groups = split(rows)
    ups, downs = width // TILE, half // TILE
    steps = ups + downs
    lanes = TILE // 2

    me = lax.axis_index("tp")
    chip, core = me // 2, me % 2
    twin = me + 1 - 2 * core
    inner, outer = ((chip + 1) // 2) % 2, chip // 2
    near, wrap = 2 * (chip + 1 - 2 * (chip % 2)) + core, 2 * (n // 2 - 1 - chip) + core
    keep, pick = (inner, outer), (outer, inner)
    peer1, peer2 = (near, wrap), (wrap, near)

    def remote(src, dst, send, recv, peer):
        return pltpu.make_async_remote_copy(
            src_ref=src, dst_ref=dst, send_sem=send, recv_sem=recv,
            device_id={"tp": peer}, device_id_type=MESH,
        )

    def tile(i):
        return pl.ds(pl.multiple_of(i * TILE, TILE), TILE)

    def far_copy(u):
        cols = pl.ds(pl.multiple_of((1 - core) * half + u * TILE, TILE), TILE)
        return remote(wd_hbm.at[:, cols], far_hbm.at[:, tile(u)], far_send.at[u], far_recv.at[u], twin)

    def x_copy(row, size):
        at = pl.multiple_of(row, 64)
        return pltpu.make_async_copy(x_hbm.at[pl.ds(at, size), :], x_buf.at[pl.ds(0, size)], x_sem)

    def up_copies(i, slot):
        return (
            pltpu.make_async_copy(wg_hbm.at[:, tile(i)], w_buf.at[slot, pl.ds(0, depth)], w_sem.at[slot, 0]),
            pltpu.make_async_copy(wu_hbm.at[:, tile(i)], w_buf.at[slot, pl.ds(depth, depth)], w_sem.at[slot, 1]),
        )

    def down_copies(u, slot):
        cols = pl.ds(pl.multiple_of(core * half + u * TILE, TILE), TILE)
        return (
            pltpu.make_async_copy(wd_hbm.at[:, cols], w_buf.at[slot, pl.ds(0, width)], w_sem.at[slot, 0]),
            pltpu.make_async_copy(far_hbm.at[:, tile(u)], w_buf.at[slot, pl.ds(width, width)], w_sem.at[slot, 1]),
        )

    def start(copies):
        for copy in copies:
            copy.start()

    def wait(copies):
        for copy in copies:
            copy.wait()

    def event(row, size, u, s):
        piece = size // 4

        def rows_of(h, q):
            return pl.multiple_of((2 * h + q) * piece, 16)

        def spot(d, h, q, count=1):
            cols = pl.multiple_of(core * half + u * TILE + d * lanes, lanes)
            return y_hbm.at[pl.ds(pl.multiple_of(row + (2 * h + q) * piece, 16), count * piece), pl.ds(cols, lanes)]

        def own(d, h, q, count=1):
            return term[u, pl.ds(rows_of(h, q), count * piece), pl.ds(d * lanes, lanes)]

        def part(d, q):
            return got1[d, u, pl.ds(pl.multiple_of(q * piece, 16), piece)].astype(F32)

        def out1(d):
            cut = pl.ds(0, 2 * piece)
            return remote(first.at[d, u, cut], got1.at[d, u, cut], send1.at[d, u], recv1.at[d, u], peer1[d])

        def out2(d):
            cut = pl.ds(0, piece)
            return remote(second.at[d, u, cut], got2.at[d, u, cut], send2.at[d, u], recv2.at[d, u], peer2[d])

        def mine(d):
            return done.at[d, u, pl.ds(0, piece)], spot(d, keep[d], pick[d])

        def back2(d):
            return remote(*mine(d), back2_send.at[d, u], back2_recv.at[d, u], peer2[d])

        def back1(d, q):
            src, dst = mine(d)
            if q:
                src = dst = spot(d, keep[d], 1 - pick[d])
            return remote(src, dst, back1_send.at[d, u, q], back1_recv.at[d, u, q], peer1[d])

        def to_twin():
            cols = pl.ds(pl.multiple_of(core * half + u * TILE, TILE), TILE)
            here = y_hbm.at[pl.ds(pl.multiple_of(row, 64), size), cols]
            return remote(here, here, late_send, late_recv, twin)

        def local(d):
            return pltpu.make_async_copy(*mine(d), local_sem.at[d, u])

        if s == 0:
            for d in range(2):
                first[d, u, pl.ds(0, 2 * piece)] = own(d, 1 - keep[d], 0, 2).astype(BF16)
            for d in range(2):
                out1(d).start()
        elif s == 1:
            for d in range(2):
                out1(d).wait_recv()
                q = 1 - pick[d]
                second[d, u, pl.ds(0, piece)] = (part(d, q) + own(d, keep[d], q)).astype(BF16)
            for d in range(2):
                out2(d).start()
        elif s == 2:
            for d in range(2):
                out2(d).wait_recv()
                total = part(d, pick[d]) + own(d, keep[d], pick[d]) + got2[d, u, pl.ds(0, piece)].astype(F32)
                done[d, u, pl.ds(0, piece)] = total.astype(BF16)
            for d in range(2):
                back2(d).start()
                back1(d, 0).start()
                local(d).start()
        elif s == 3:
            for d in range(2):
                back2(d).wait_recv()
                back1(d, 1).start()
        else:
            for d in range(2):
                back1(d, 0).wait_recv()
                back1(d, 1).wait_recv()
                local(d).wait()
            to_twin().start()
            for d in range(2):
                out1(d).wait_send()
                out2(d).wait_send()
                back2(d).wait_send()
                back1(d, 0).wait_send()
                back1(d, 1).wait_send()

    def gap_of(size):
        return LAST_GAP if size == groups[-1][0] else GAP

    def events(row, size, tau):
        for s in range(4, -1, -1):
            u = tau - gap_of(size) * s

            @pl.when((u >= 0) & (u < downs))
            def _(u=u, s=s):
                event(row, size, u, s)

    def chunk(k, row, size, before, after):
        x_copy(row, size).wait()
        par = k % 2
        base = k * steps
        here = pl.ds(0, size)

        def hid_copy(i):
            return remote(
                hid.at[here, tile(i)], far_hid.at[par, here, tile(i)], hid_send.at[par], hid_recv.at[par], twin
            )

        def next_down(u, slot):
            @pl.when(k == 0)
            def _():
                far_copy(u).wait()

            start(down_copies(u, slot))

        def up_body(i, _):
            slot = (base + i) % 2
            wait(up_copies(i, slot))

            @pl.when(i < ups - 1)
            def _():
                start(up_copies(i + 1, 1 - slot))

            @pl.when(i == ups - 1)
            def _():
                next_down(0, 1 - slot)

            gate = jnp.dot(x_buf[here], w_buf[slot, pl.ds(0, depth)], preferred_element_type=F32)
            up = jnp.dot(x_buf[here], w_buf[slot, pl.ds(depth, depth)], preferred_element_type=F32)
            hid[here, tile(i)] = (jax.nn.silu(gate) * up).astype(BF16)
            before(i + downs)
            hid_copy(i).start()
            return _

        lax.fori_loop(0, ups, up_body, None)

        def down_step(u, lead):
            slot = (base + ups + u) % 2
            wait(down_copies(u, slot))
            if lead:
                next_down(u + 1, 1 - slot)
                if after is not None:
                    after()
                term[u, here] = jnp.dot(
                    hid[here], w_buf[slot, pl.ds(0, width)], preferred_element_type=F32
                )
                remote(
                    hid.at[here], far_hid.at[par, here], hid_send.at[par], hid_recv.at[par], twin,
                ).wait()
                term[u, here] += jnp.dot(
                    far_hid[par, here], w_buf[slot, pl.ds(width, width)], preferred_element_type=F32
                )
            else:
                @pl.when(u < downs - 1)
                def _():
                    next_down(u + 1, 1 - slot)

                if after is not None:
                    @pl.when(u == downs - 1)
                    def _():
                        start(up_copies(0, 1 - slot))

                term[u, here] = jnp.dot(
                    hid[here], w_buf[slot, pl.ds(0, width)], preferred_element_type=F32
                ) + jnp.dot(
                    far_hid[par, here], w_buf[slot, pl.ds(width, width)], preferred_element_type=F32
                )
            before(steps + u)
            events(row, size, u)

        down_step(0, True)

        def down_body(u, _):
            down_step(u, False)
            return _

        lax.fori_loop(1, downs, down_body, None)

    x_copy(0, groups[0][0]).start()
    start(up_copies(0, 0))
    barrier = pltpu.get_barrier_semaphore()
    for peer in (near, wrap, twin):
        pl.semaphore_signal(barrier, inc=1, device_id={"tp": peer}, device_id_type=MESH)
    pl.semaphore_wait(barrier, 3)
    for u in range(downs):
        far_copy(u).start()

    def idle(tau):
        return

    first_chunk, row, before = 0, 0, idle
    for g, (size, count) in enumerate(groups):
        later = groups[g + 1][0] if g + 1 < len(groups) else None

        def one(k, at, first_in_group, before=before, size=size, later=later, end=first_chunk + count - 1):
            def after():
                if later is None:
                    if count > 1:
                        @pl.when(k < end)
                        def _():
                            x_copy(at + size, size).start()
                    return

                @pl.when(k < end)
                def _():
                    x_copy(at + size, size).start()

                @pl.when(k == end)
                def _():
                    x_copy(at + size, later).start()

            chunk(k, at, size, before, None if later is None and count == 1 else after)

        if count == 1:
            one(first_chunk, row, True)
        else:
            assert g == 0

            def body(k, _, size=size, one=one):
                at = k * size

                def before(tau):
                    @pl.when(k > 0)
                    def _():
                        events(at - size, size, tau)

                one(k, at, False, before=before)
                return _

            lax.fori_loop(0, count, body, None)
        row += size * count
        first_chunk += count
        before = functools.partial(events, row - size, size)

    def tail(tau, _):
        before(tau)
        return _

    lax.fori_loop(downs, downs + 4 * LAST_GAP, tail, None)

    whole = y_hbm.at[:, pl.ds(0, half)]
    pltpu.make_async_copy(whole, whole, late_send).wait()
    pltpu.make_async_copy(whole, whole, late_recv).wait()


def copy_kernel(src, dst, buf, read_sem, write_sem):
    size = src.shape[0] // BLOCKS

    def read(i):
        return pltpu.make_async_copy(src.at[pl.ds(i * size, size)], buf.at[i], read_sem.at[i])

    def write(i):
        return pltpu.make_async_copy(buf.at[i], dst.at[pl.ds(i * size, size)], write_sem.at[i])

    for i in range(BLOCKS):
        read(i).start()
    for i in range(BLOCKS):
        read(i).wait()
        write(i).start()
    for i in range(BLOCKS):
        write(i).wait()


def solution(mesh):
    n = mesh.shape["tp"]

    def step(x, w_gate, w_up, w_down):
        rows, depth = x.shape
        width = w_gate.shape[1]
        half = depth // 2
        downs = half // TILE
        big = max(split(rows))[0]
        piece, lanes = big // 4, TILE // 2
        dma = pltpu.SemaphoreType.DMA
        y, _ = pl.pallas_call(
            functools.partial(kernel, n),
            name="mlp",
            out_shape=(
                jax.ShapeDtypeStruct((rows, depth), BF16),
                jax.ShapeDtypeStruct((width, half), BF16),
            ),
            in_specs=[pl.BlockSpec(memory_space=pl.ANY)] * 4,
            out_specs=[pl.BlockSpec(memory_space=pl.ANY)] * 2,
            scratch_shapes=[
                pltpu.VMEM((big, depth), BF16),
                pltpu.VMEM((2, 2 * depth, TILE), BF16),
                pltpu.VMEM((big, width), BF16),
                pltpu.VMEM((2, big, width), BF16),
                pltpu.VMEM((downs, big, TILE), F32),
                pltpu.VMEM((2, downs, 2 * piece, lanes), BF16),
                pltpu.VMEM((2, downs, 2 * piece, lanes), BF16),
                pltpu.VMEM((2, downs, piece, lanes), BF16),
                pltpu.VMEM((2, downs, piece, lanes), BF16),
                pltpu.VMEM((2, downs, piece, lanes), BF16),
                dma,
                dma((2, 2)),
                dma((downs,)),
                dma((downs,)),
                dma((2,)),
                dma((2,)),
                dma((2, downs)),
                dma((2, downs)),
                dma((2, downs)),
                dma((2, downs)),
                dma((2, downs)),
                dma((2, downs)),
                dma((2, downs, 2)),
                dma((2, downs, 2)),
                dma((2, downs)),
                dma,
                dma,
            ],
            compiler_params=pltpu.CompilerParams(
                collective_id=0, has_side_effects=True, vmem_limit_bytes=67_043_328
            ),
            cost_estimate=pl.CostEstimate(
                flops=6 * rows * depth * width,
                bytes_accessed=2 * (2 * rows * depth + 12 * depth * width),
                transcendentals=rows * width,
            ),
        )(x, w_gate, w_up, w_down)
        return pl.pallas_call(
            copy_kernel,
            name="hand_over",
            out_shape=jax.ShapeDtypeStruct((rows, depth), BF16),
            in_specs=[pl.BlockSpec(memory_space=pl.ANY)],
            out_specs=pl.BlockSpec(memory_space=pl.ANY),
            scratch_shapes=[pltpu.VMEM((BLOCKS, rows // BLOCKS, depth), BF16), dma((BLOCKS,)), dma((BLOCKS,))],
            compiler_params=pltpu.CompilerParams(vmem_limit_bytes=67_043_328),
            cost_estimate=pl.CostEstimate(flops=0, bytes_accessed=4 * rows * depth, transcendentals=0),
        )(y)

    return jax.shard_map(
        step,
        mesh=mesh,
        in_specs=(P("dp", None), P(None, "tp"), P(None, "tp"), P("tp", None)),
        out_specs=P("dp", None),
        check_vma=False,
    )
```

```python
import functools

import jax
import jax.numpy as jnp
from jax import lax
from jax.experimental import pallas as pl
from jax.experimental.pallas import tpu as pltpu
from jax.sharding import PartitionSpec as P

TILE = 512
MESH = pl.DeviceIdType.MESH
F32, BF16 = jnp.float32, jnp.bfloat16


SHARES = ((9, 2), (8, 1), (6, 1))
BLOCKS = 16
GAP, LAST_GAP = 3, 3


def split(rows):
    return [(rows * share // 32, count) for share, count in SHARES]


def kernel(
    n, x_hbm, wg_hbm, wu_hbm, wd_hbm, y_hbm, far_hbm,
    x_buf, w_buf, hid, far_hid, term, first, got1, second, got2, done, act,
    x_sem, w_sem, far_send, far_recv, hid_send, hid_recv,
    send1, recv1, send2, recv2, back2_send, back2_recv, back1_send, back1_recv,
    local_sem, late_send, late_recv,
):
    rows, depth = x_hbm.shape
    width = wg_hbm.shape[1]
    half = depth // 2
    groups = split(rows)
    ups, downs = width // TILE, half // TILE
    steps = ups + downs
    lanes = TILE // 2

    me = lax.axis_index("tp")
    chip, core = me // 2, me % 2
    twin = me + 1 - 2 * core
    inner, outer = ((chip + 1) // 2) % 2, chip // 2
    near, wrap = 2 * (chip + 1 - 2 * (chip % 2)) + core, 2 * (n // 2 - 1 - chip) + core
    keep, pick = (inner, outer), (outer, inner)
    peer1, peer2 = (near, wrap), (wrap, near)

    def remote(src, dst, send, recv, peer):
        return pltpu.make_async_remote_copy(
            src_ref=src, dst_ref=dst, send_sem=send, recv_sem=recv,
            device_id={"tp": peer}, device_id_type=MESH,
        )

    def tile(i):
        return pl.ds(pl.multiple_of(i * TILE, TILE), TILE)

    def far_copy(u):
        cols = pl.ds(pl.multiple_of((1 - core) * half + u * TILE, TILE), TILE)
        return remote(wd_hbm.at[:, cols], far_hbm.at[:, tile(u)], far_send.at[u], far_recv.at[u], twin)

    def x_copy(row, size):
        at = pl.multiple_of(row, 64)
        return pltpu.make_async_copy(x_hbm.at[pl.ds(at, size), :], x_buf.at[pl.ds(0, size)], x_sem)

    def up_copies(i, slot):
        return (
            pltpu.make_async_copy(wg_hbm.at[:, tile(i)], w_buf.at[slot, pl.ds(0, depth)], w_sem.at[slot, 0]),
            pltpu.make_async_copy(wu_hbm.at[:, tile(i)], w_buf.at[slot, pl.ds(depth, depth)], w_sem.at[slot, 1]),
        )

    def down_copies(u, slot):
        cols = pl.ds(pl.multiple_of(core * half + u * TILE, TILE), TILE)
        return (
            pltpu.make_async_copy(wd_hbm.at[:, cols], w_buf.at[slot, pl.ds(0, width)], w_sem.at[slot, 0]),
            pltpu.make_async_copy(far_hbm.at[:, tile(u)], w_buf.at[slot, pl.ds(width, width)], w_sem.at[slot, 1]),
        )

    def start(copies):
        for copy in copies:
            copy.start()

    def wait(copies):
        for copy in copies:
            copy.wait()

    def event(row, size, u, s):
        piece = size // 4

        def rows_of(h, q):
            return pl.multiple_of((2 * h + q) * piece, 16)

        def spot(d, h, q, count=1):
            cols = pl.multiple_of(core * half + u * TILE + d * lanes, lanes)
            return y_hbm.at[pl.ds(pl.multiple_of(row + (2 * h + q) * piece, 16), count * piece), pl.ds(cols, lanes)]

        def own(d, h, q, count=1):
            return term[u, pl.ds(rows_of(h, q), count * piece), pl.ds(d * lanes, lanes)]

        def part(d, q):
            return got1[d, u, pl.ds(pl.multiple_of(q * piece, 16), piece)].astype(F32)

        def out1(d):
            cut = pl.ds(0, 2 * piece)
            return remote(first.at[d, u, cut], got1.at[d, u, cut], send1.at[d, u], recv1.at[d, u], peer1[d])

        def out2(d):
            cut = pl.ds(0, piece)
            return remote(second.at[d, u, cut], got2.at[d, u, cut], send2.at[d, u], recv2.at[d, u], peer2[d])

        def mine(d):
            return done.at[d, u, pl.ds(0, piece)], spot(d, keep[d], pick[d])

        def back2(d):
            return remote(*mine(d), back2_send.at[d, u], back2_recv.at[d, u], peer2[d])

        def back1(d, q):
            src, dst = mine(d)
            if q:
                src = dst = spot(d, keep[d], 1 - pick[d])
            return remote(src, dst, back1_send.at[d, u, q], back1_recv.at[d, u, q], peer1[d])

        def to_twin():
            cols = pl.ds(pl.multiple_of(core * half + u * TILE, TILE), TILE)
            here = y_hbm.at[pl.ds(pl.multiple_of(row, 64), size), cols]
            return remote(here, here, late_send, late_recv, twin)

        def local(d):
            return pltpu.make_async_copy(*mine(d), local_sem.at[d, u])

        if s == 0:
            for d in range(2):
                first[d, u, pl.ds(0, 2 * piece)] = own(d, 1 - keep[d], 0, 2).astype(BF16)
            for d in range(2):
                out1(d).start()
        elif s == 1:
            for d in range(2):
                out1(d).wait_recv()
                q = 1 - pick[d]
                second[d, u, pl.ds(0, piece)] = (part(d, q) + own(d, keep[d], q)).astype(BF16)
            for d in range(2):
                out2(d).start()
        elif s == 2:
            for d in range(2):
                out2(d).wait_recv()
                total = part(d, pick[d]) + own(d, keep[d], pick[d]) + got2[d, u, pl.ds(0, piece)].astype(F32)
                done[d, u, pl.ds(0, piece)] = total.astype(BF16)
            for d in range(2):
                back2(d).start()
                back1(d, 0).start()
                local(d).start()
        elif s == 3:
            for d in range(2):
                back2(d).wait_recv()
                back1(d, 1).start()
        else:
            for d in range(2):
                back1(d, 0).wait_recv()
                back1(d, 1).wait_recv()
                local(d).wait()
            to_twin().start()
            for d in range(2):
                out1(d).wait_send()
                out2(d).wait_send()
                back2(d).wait_send()
                back1(d, 0).wait_send()
                back1(d, 1).wait_send()

    def gap_of(size):
        return LAST_GAP if size == groups[-1][0] else GAP

    def events(row, size, tau):
        for s in range(4, -1, -1):
            u = tau - gap_of(size) * s

            @pl.when((u >= 0) & (u < downs))
            def _(u=u, s=s):
                event(row, size, u, s)

    def chunk(k, row, size, before, after):
        x_copy(row, size).wait()
        par = k % 2
        base = k * steps
        here = pl.ds(0, size)

        def hid_copy(i):
            return remote(
                hid.at[here, tile(i)], far_hid.at[par, here, tile(i)], hid_send.at[par], hid_recv.at[par], twin
            )

        def next_down(u, slot):
            @pl.when(k == 0)
            def _():
                far_copy(u).wait()

            start(down_copies(u, slot))

        def up_body(i, _):
            slot = (base + i) % 2
            wait(up_copies(i, slot))

            @pl.when(i < ups - 1)
            def _():
                start(up_copies(i + 1, 1 - slot))

            @pl.when(i == ups - 1)
            def _():
                next_down(0, 1 - slot)

            gate = jnp.dot(x_buf[here], w_buf[slot, pl.ds(0, depth)], preferred_element_type=F32)
            act[here] = jax.nn.silu(gate)
            up = jnp.dot(x_buf[here], w_buf[slot, pl.ds(depth, depth)], preferred_element_type=F32)
            hid[here, tile(i)] = (act[here] * up).astype(BF16)
            before(i + downs)
            hid_copy(i).start()
            return _

        lax.fori_loop(0, ups, up_body, None)

        def down_step(u, lead):
            slot = (base + ups + u) % 2
            wait(down_copies(u, slot))
            if lead:
                next_down(u + 1, 1 - slot)
                if after is not None:
                    after()
                term[u, here] = jnp.dot(
                    hid[here], w_buf[slot, pl.ds(0, width)], preferred_element_type=F32
                )
                remote(
                    hid.at[here], far_hid.at[par, here], hid_send.at[par], hid_recv.at[par], twin,
                ).wait()
                term[u, here] += jnp.dot(
                    far_hid[par, here], w_buf[slot, pl.ds(width, width)], preferred_element_type=F32
                )
            else:
                @pl.when(u < downs - 1)
                def _():
                    next_down(u + 1, 1 - slot)

                if after is not None:
                    @pl.when(u == downs - 1)
                    def _():
                        start(up_copies(0, 1 - slot))

                term[u, here] = jnp.dot(
                    hid[here], w_buf[slot, pl.ds(0, width)], preferred_element_type=F32
                ) + jnp.dot(
                    far_hid[par, here], w_buf[slot, pl.ds(width, width)], preferred_element_type=F32
                )
            before(steps + u)
            events(row, size, u)

        down_step(0, True)

        def down_body(u, _):
            down_step(u, False)
            return _

        lax.fori_loop(1, downs, down_body, None)

    x_copy(0, groups[0][0]).start()
    start(up_copies(0, 0))
    barrier = pltpu.get_barrier_semaphore()
    for peer in (near, wrap, twin):
        pl.semaphore_signal(barrier, inc=1, device_id={"tp": peer}, device_id_type=MESH)
    pl.semaphore_wait(barrier, 3)
    for u in range(downs):
        far_copy(u).start()

    def idle(tau):
        return

    first_chunk, row, before = 0, 0, idle
    for g, (size, count) in enumerate(groups):
        later = groups[g + 1][0] if g + 1 < len(groups) else None

        def one(k, at, first_in_group, before=before, size=size, later=later, end=first_chunk + count - 1):
            def after():
                if later is None:
                    if count > 1:
                        @pl.when(k < end)
                        def _():
                            x_copy(at + size, size).start()
                    return

                @pl.when(k < end)
                def _():
                    x_copy(at + size, size).start()

                @pl.when(k == end)
                def _():
                    x_copy(at + size, later).start()

            chunk(k, at, size, before, None if later is None and count == 1 else after)

        if count == 1:
            one(first_chunk, row, True)
        else:
            assert g == 0

            def body(k, _, size=size, one=one):
                at = k * size

                def before(tau):
                    @pl.when(k > 0)
                    def _():
                        events(at - size, size, tau)

                one(k, at, False, before=before)
                return _

            lax.fori_loop(0, count, body, None)
        row += size * count
        first_chunk += count
        before = functools.partial(events, row - size, size)

    def tail(tau, _):
        before(tau)
        return _

    lax.fori_loop(downs, downs + 4 * LAST_GAP, tail, None)

    whole = y_hbm.at[:, pl.ds(0, half)]
    pltpu.make_async_copy(whole, whole, late_send).wait()
    pltpu.make_async_copy(whole, whole, late_recv).wait()


def copy_kernel(src, dst, buf, read_sem, write_sem):
    size = src.shape[0] // BLOCKS

    def read(i):
        return pltpu.make_async_copy(src.at[pl.ds(i * size, size)], buf.at[i], read_sem.at[i])

    def write(i):
        return pltpu.make_async_copy(buf.at[i], dst.at[pl.ds(i * size, size)], write_sem.at[i])

    for i in range(BLOCKS):
        read(i).start()
    for i in range(BLOCKS):
        read(i).wait()
        write(i).start()
    for i in range(BLOCKS):
        write(i).wait()


def solution(mesh):
    n = mesh.shape["tp"]

    def step(x, w_gate, w_up, w_down):
        rows, depth = x.shape
        width = w_gate.shape[1]
        half = depth // 2
        downs = half // TILE
        big = max(split(rows))[0]
        piece, lanes = big // 4, TILE // 2
        dma = pltpu.SemaphoreType.DMA
        y, _ = pl.pallas_call(
            functools.partial(kernel, n),
            name="mlp",
            out_shape=(
                jax.ShapeDtypeStruct((rows, depth), BF16),
                jax.ShapeDtypeStruct((width, half), BF16),
            ),
            in_specs=[pl.BlockSpec(memory_space=pl.ANY)] * 4,
            out_specs=[pl.BlockSpec(memory_space=pl.ANY)] * 2,
            scratch_shapes=[
                pltpu.VMEM((big, depth), BF16),
                pltpu.VMEM((2, 2 * depth, TILE), BF16),
                pltpu.VMEM((big, width), BF16),
                pltpu.VMEM((2, big, width), BF16),
                pltpu.VMEM((downs, big, TILE), F32),
                pltpu.VMEM((2, downs, 2 * piece, lanes), BF16),
                pltpu.VMEM((2, downs, 2 * piece, lanes), BF16),
                pltpu.VMEM((2, downs, piece, lanes), BF16),
                pltpu.VMEM((2, downs, piece, lanes), BF16),
                pltpu.VMEM((2, downs, piece, lanes), BF16),
                pltpu.VMEM((big, TILE), F32),
                dma,
                dma((2, 2)),
                dma((downs,)),
                dma((downs,)),
                dma((2,)),
                dma((2,)),
                dma((2, downs)),
                dma((2, downs)),
                dma((2, downs)),
                dma((2, downs)),
                dma((2, downs)),
                dma((2, downs)),
                dma((2, downs, 2)),
                dma((2, downs, 2)),
                dma((2, downs)),
                dma,
                dma,
            ],
            compiler_params=pltpu.CompilerParams(
                collective_id=0, has_side_effects=True, vmem_limit_bytes=67_043_328
            ),
            cost_estimate=pl.CostEstimate(
                flops=6 * rows * depth * width,
                bytes_accessed=2 * (2 * rows * depth + 12 * depth * width),
                transcendentals=rows * width,
            ),
        )(x, w_gate, w_up, w_down)
        return pl.pallas_call(
            copy_kernel,
            name="hand_over",
            out_shape=jax.ShapeDtypeStruct((rows, depth), BF16),
            in_specs=[pl.BlockSpec(memory_space=pl.ANY)],
            out_specs=pl.BlockSpec(memory_space=pl.ANY),
            scratch_shapes=[pltpu.VMEM((BLOCKS, rows // BLOCKS, depth), BF16), dma((BLOCKS,)), dma((BLOCKS,))],
            compiler_params=pltpu.CompilerParams(vmem_limit_bytes=67_043_328),
            cost_estimate=pl.CostEstimate(flops=0, bytes_accessed=4 * rows * depth, transcendentals=0),
        )(y)

    return jax.shard_map(
        step,
        mesh=mesh,
        in_specs=(P("dp", None), P(None, "tp"), P(None, "tp"), P("tp", None)),
        out_specs=P("dp", None),
        check_vma=False,
    )
```
